16 devices in a mesh: rep: 2 (over y, z), pp: 8 (over x, core).
Axes of the slice: x: 4, y: 2, z: 1, core: 2. Of those that a mesh axis runs over, the one named last changes fastest.
The devices are a block of a 4x4x8 slice.
Arguments:
- x: bfloat16 [32, 512, 640], P('rep'), parts along dimension 0
- dy: bfloat16 [32, 512, 640], P('rep'), parts along dimension 0
- w_gate: bfloat16 [8, 640, 1536], P('pp')
- w_up: bfloat16 [8, 640, 1536], P('pp')
- w_down: bfloat16 [8, 1536, 640], P('pp')
Outputs:
- output 1: bfloat16 [16, 640, 1536], P(('rep', 'pp')), parts along dimension 0
- output 2: bfloat16 [16, 640, 1536], P(('rep', 'pp')), parts along dimension 0
- output 3: bfloat16 [16, 1536, 640], P(('rep', 'pp')), parts along dimension 0
There are 2 independent parts. The reference program is written for one: setup_inputs(seed, part) draws one part's arguments, and reference() takes and returns one part's arrays. A program takes and returns all parts, laid end to end along the dimension named above; an argument that names none is the same for every part.
All inputs are finite; a program needn't handle non-finite values.
Results may differ from the reference program's by a relative error of at most 0.0307.
Values are sent between devices in bfloat16 or wider.
A program may use at most 768 MiB of HBM per device.

```python
import jax
import jax.numpy as jnp
from jax import lax

MICRO = 16
TOKENS = 512
D = 640
FF = 1536
LAYERS = 8
NAMES = ("w_gate", "w_up", "w_down")
SHAPES = {"w_gate": (LAYERS, D, FF), "w_up": (LAYERS, D, FF), "w_down": (LAYERS, FF, D)}


def bump(key, n, height):
    away = (jnp.arange(n, dtype=jnp.int32) - jax.random.randint(key, (), 0, n, jnp.int32)) % n
    return jnp.where(away < n // 8, height, 1.0)


def together(key, own, strength):
    shared = jax.random.normal(key, own.shape[1:], jnp.float32)
    return (own + strength * shared) * lax.rsqrt(1 + strength * strength)


def setup_inputs(seed: int = 0, part: int = 0) -> dict:
    kx, kdy, ka, kb, kz, kf, kh, kl, *kw = jax.random.split(jax.random.key(seed), 8 + len(NAMES))
    kx, kdy, ka, kb = (jax.random.fold_in(k, part) for k in (kx, kdy, ka, kb))
    shape = (MICRO, TOKENS, D)
    much_x, much_dy = jax.random.uniform(kz, (2,), jnp.float32, 0.0, 1.0)
    layers = 2.0 ** jax.random.uniform(kl, (LAYERS, 1, 1), jnp.float32, -1.0, 1.0)
    x = together(ka, jax.random.normal(kx, shape, jnp.float32), much_x) * bump(kf, D, 4.0)
    dy = together(kb, jax.random.normal(kdy, shape, jnp.float32), much_dy)
    drawn = {"x": x.astype(jnp.bfloat16), "dy": (dy * (MICRO * TOKENS) ** -0.5).astype(jnp.bfloat16)}
    for key, name in zip(kw, NAMES, strict=True):
        w = jax.random.normal(key, SHAPES[name], jnp.float32) * SHAPES[name][1] ** -0.5
        drawn[name] = (w * {"w_gate": 1.0, "w_up": bump(kh, FF, 4.0), "w_down": layers}[name]).astype(jnp.bfloat16)
    return drawn


def matmul(a, w):
    return jnp.dot(a, w, preferred_element_type=jnp.float32).astype(jnp.bfloat16)


def normed(h):
    wide = h.astype(jnp.float32)
    scale = lax.rsqrt(jnp.mean(wide**2, -1, keepdims=True) + 1e-6)
    return (wide * scale).astype(jnp.bfloat16)


def layer(h, w):
    a = normed(h)
    gate = jnp.dot(a, w["w_gate"], preferred_element_type=jnp.float32)
    up = jnp.dot(a, w["w_up"], preferred_element_type=jnp.float32)
    return h + matmul((jax.nn.silu(gate) * up).astype(jnp.bfloat16), w["w_down"])


def stack(weights, h):
    return lax.scan(lambda h, w: (layer(h, w), None), h, weights)[0]


def reference(x, dy, w_gate, w_up, w_down):
    weights = dict(zip(NAMES, (w_gate, w_up, w_down), strict=True))

    def take(so_far, one):
        h, by_y = one
        _, back = jax.vjp(lambda w: stack(w, h), weights)
        return jax.tree.map(lambda total, term: total + term.astype(jnp.float32), so_far, back(by_y)[0]), None

    none_yet = {name: jnp.zeros(w.shape, jnp.float32) for name, w in weights.items()}
    by_weights, _ = lax.scan(take, none_yet, (x, dy))
    return tuple(by_weights[name].astype(jnp.bfloat16) for name in NAMES)
```

```python
import functools

import jax
import jax.numpy as jnp
from jax import lax
from jax.experimental import pallas as pl
from jax.experimental.pallas import tpu as pltpu
from jax.sharding import PartitionSpec as P

C = 2
NH = 8
NG = 4
ND = 2
TN = 512
EPS = 1e-6


def dot(a, b):
    return jnp.dot(a, b, preferred_element_type=jnp.float32)


def kernel(stages, x_hbm, dy_hbm, wg_hbm, wu_hbm, wd_hbm, og_hbm, ou_hbm, od_hbm, spill, wg, wu, wd, wgt, wut, wdt, tg, tu, td, hbuf, gbuf, fsend,
           bsend, keep, back, a_v, act_v, sg, su, sa, at, dt, wsem, xsem, ysem, frecv, fsent, brecv, bsent, keepsem, backsem, fcred, bcred):
    micro, _, rows, d = x_hbm.shape
    ff = wg.shape[1]
    me = lax.axis_index("pp")
    first, last = me == 0, me == stages - 1
    warm = jnp.minimum(stages - me, NH - 1)

    loads = [pltpu.make_async_copy(src.at[0], dst, wsem.at[i]) for i, (src, dst) in enumerate(((wg_hbm, wg), (wu_hbm, wu), (wd_hbm, wd)))]
    for load in loads:
        load.start()

    def x_copy(m):
        return pltpu.make_async_copy(x_hbm.at[m], hbuf.at[lax.rem(m, NH)], xsem)

    def dy_copy(m):
        return pltpu.make_async_copy(dy_hbm.at[m], gbuf.at[lax.rem(m, NG)], ysem)

    @pl.when(first)
    def _():
        x_copy(0).start()

    @pl.when(last)
    def _():
        dy_copy(0).start()

    barrier = pltpu.get_barrier_semaphore()

    @pl.when(me > 0)
    def _():
        pl.semaphore_signal(barrier, inc=1, device_id={"pp": me - 1})

    @pl.when(me < stages - 1)
    def _():
        pl.semaphore_signal(barrier, inc=1, device_id={"pp": me + 1})

    pl.semaphore_wait(barrier, jnp.where(first | last, 1, 2))

    def f_copy(m, c):
        out, slot = lax.rem(m, 2) * C + c, lax.rem(m, NH)
        return pltpu.make_async_remote_copy(
            src_ref=fsend.at[out], dst_ref=hbuf.at[slot, c], send_sem=fsent.at[out], recv_sem=frecv.at[slot * C + c], device_id={"pp": me + 1}
        )

    def b_copy(m, c):
        out, slot = lax.rem(m, 2) * C + c, lax.rem(m, NG)
        return pltpu.make_async_remote_copy(
            src_ref=bsend.at[out], dst_ref=gbuf.at[slot, c], send_sem=bsent.at[out], recv_sem=brecv.at[slot * C + c], device_id={"pp": me - 1}
        )

    def keep_copy(m, c):
        return pltpu.make_async_copy(keep.at[c], spill.at[m, c], keepsem.at[c])

    def back_copy(m, c):
        return pltpu.make_async_copy(spill.at[m, c], back.at[c], backsem.at[c])

    def norm(h):
        wide = h.astype(jnp.float32)
        scale = lax.rsqrt(jnp.mean(wide * wide, -1, keepdims=True) + EPS)
        return wide, scale

    def tiles(body, width=TN, total=ff):
        def one(n, _):
            body(pl.ds(pl.multiple_of(n * width, width), width))
            return 0

        lax.fori_loop(0, total // width, one, 0)

    for load in loads:
        load.wait()

    def forward(m):
        slot = lax.rem(m, NH)

        @pl.when(first)
        def _():
            x_copy(m).wait()

            @pl.when(m + 1 < micro)
            def _():
                x_copy(m + 1).start()

        @pl.when(jnp.logical_not(last) & (m >= NH))
        def _():
            pl.semaphore_wait(fcred, 1)

        def chunk(c, _):
            @pl.when(me > 0)
            def _():
                f_copy(m, c).wait_recv()

            wide, scale = norm(hbuf[slot, c])
            a_v[...] = (wide * scale).astype(jnp.bfloat16)

            def tile(n):
                gate = dot(a_v[...], wg[:, n])
                keep[c, 0, :, n] = gate
                up = dot(a_v[...], wu[:, n])
                keep[c, 1, :, n] = up
                act_v[:, n] = ((gate * jax.nn.sigmoid(gate)) * up).astype(jnp.bfloat16)

            tiles(tile)
            keep_copy(m, c).start()

            @pl.when(me < stages - 1)
            def _():
                @pl.when(m >= 2)
                def _():
                    f_copy(m - 2, c).wait_send()

                out = lax.rem(m, 2) * C + c
                fsend[out] = hbuf[slot, c] + dot(act_v[...], wd[...]).astype(jnp.bfloat16)
                f_copy(m, c).start()

            return 0

        lax.fori_loop(0, C, chunk, 0)

    def backward(m):
        slot, hslot, q = lax.rem(m, NG), lax.rem(m, NH), lax.rem(m, ND)

        @pl.when(last)
        def _():
            dy_copy(m).wait()

            @pl.when(m + 1 < micro)
            def _():
                dy_copy(m + 1).start()

        @pl.when((me > 0) & (m >= NG))
        def _():
            pl.semaphore_wait(bcred, 1)

        def chunk(c, _):
            r = pl.ds(pl.multiple_of(c * rows, rows), rows)

            @pl.when(me < stages - 1)
            def _():
                b_copy(m, c).wait_recv()

            back_copy(m, c).wait()

            def tile(n):
                by_act = dot(gbuf[slot, c], wdt[:, n]).astype(jnp.bfloat16).astype(jnp.float32)
                gate, up = back[c, 0, :, n], back[c, 1, :, n]
                s = jax.nn.sigmoid(gate)
                silu = gate * s
                sa[q, r, n] = (silu * up).astype(jnp.bfloat16)
                su[q, r, n] = (by_act * silu).astype(jnp.bfloat16)
                sg[q, r, n] = ((by_act * up) * (s + silu * (1.0 - s))).astype(jnp.bfloat16)

            tiles(tile)
            wide, scale = norm(hbuf[hslot, c])
            at[q, :, r] = (wide * scale).astype(jnp.bfloat16).T
            dt[q, :, r] = gbuf[slot, c].T

            @pl.when(me > 0)
            def _():
                @pl.when(m >= 2)
                def _():
                    b_copy(m - 2, c).wait_send()

                by_a = dot(sg[q, r, :], wgt[...]).astype(jnp.bfloat16) + dot(su[q, r, :], wut[...]).astype(jnp.bfloat16)
                by_a = by_a.astype(jnp.float32)
                wide, scale = norm(hbuf[hslot, c])
                by_scale = jnp.sum(by_a * wide, -1, keepdims=True)
                by_wide = by_a * scale - wide * (by_scale * (scale * scale * scale) * (1.0 / d))
                bsend[lax.rem(m, 2) * C + c] = by_wide.astype(jnp.bfloat16) + gbuf[slot, c]
                b_copy(m, c).start()

            return 0

        lax.fori_loop(0, C, chunk, 0)

        @pl.when((me > 0) & (m + NH < micro))
        def _():
            pl.semaphore_signal(fcred, inc=1, device_id={"pp": me - 1})

        @pl.when((me < stages - 1) & (m + NG < micro))
        def _():
            pl.semaphore_signal(bcred, inc=1, device_id={"pp": me + 1})

    def term(total, left, right):
        def tile(n):
            total[:, n] += dot(left, right[:, n]).astype(jnp.bfloat16).astype(jnp.float32)

        tiles(tile)

    def step(t, _):
        f, b = t, t - warm
        w = b - (ND - 1)
        q = lax.rem(w + ND * micro, ND)
        f_on, w_on = f < micro, (w >= 0) & (w < micro)

        @pl.when((b >= 0) & (b < micro))
        def _():
            backward(b)

        @pl.when(f_on)
        def _():
            forward(f)

        @pl.when(w_on)
        def _():
            term(tg, at[q], sg.at[q])

        @pl.when(f_on)
        def _():
            for c in range(C):
                keep_copy(f, c).wait()

        @pl.when((b + 1 >= 0) & (b + 1 < micro))
        def _():
            for c in range(C):
                back_copy(b + 1, c).start()

        @pl.when(w_on)
        def _():
            term(tu, at[q], su.at[q])
            term(td, dt[q], sa.at[q])

        return 0

    wgt[...] = wg[...].T
    wut[...] = wu[...].T
    wdt[...] = wd[...].T
    for total in (tg, tu, td):
        total[...] = jnp.zeros_like(total)

    lax.fori_loop(0, micro + NH - 1 + ND - 1, step, 0)

    for m in (micro - 2, micro - 1):
        for c in range(C):
            @pl.when(me < stages - 1)
            def _():
                f_copy(m, c).wait_send()

            @pl.when(me > 0)
            def _():
                b_copy(m, c).wait_send()

    wg[...] = tg[...].astype(jnp.bfloat16)
    wu[...] = tu[...].astype(jnp.bfloat16)
    wd[...] = td[...].astype(jnp.bfloat16).T
    stores = [pltpu.make_async_copy(src, dst.at[0], wsem.at[i]) for i, (src, dst) in enumerate(((wg, og_hbm), (wu, ou_hbm), (wd, od_hbm)))]
    for store in stores:
        store.start()
    for store in stores:
        store.wait()


def solution(mesh):
    stages = mesh.shape["pp"]

    def step(x, dy, w_gate, w_up, w_down):
        micro, tokens, d = x.shape
        ff = w_gate.shape[2]
        rows = tokens // C
        bf16, f32 = jnp.bfloat16, jnp.float32
        anywhere = pl.BlockSpec(memory_space=pl.ANY)
        dma = pltpu.SemaphoreType.DMA
        outs = pl.pallas_call(
            functools.partial(kernel, stages),
            out_shape=(
                jax.ShapeDtypeStruct(w_gate.shape, bf16),
                jax.ShapeDtypeStruct(w_up.shape, bf16),
                jax.ShapeDtypeStruct(w_down.shape, bf16),
                jax.ShapeDtypeStruct((micro, C, 2, rows, ff), f32),
            ),
            in_specs=[anywhere] * 5,
            out_specs=(anywhere,) * 4,
            scratch_shapes=[
                pltpu.VMEM((d, ff), bf16),
                pltpu.VMEM((d, ff), bf16),
                pltpu.VMEM((ff, d), bf16),
                pltpu.VMEM((ff, d), bf16),
                pltpu.VMEM((ff, d), bf16),
                pltpu.VMEM((d, ff), bf16),
                pltpu.VMEM((d, ff), f32),
                pltpu.VMEM((d, ff), f32),
                pltpu.VMEM((d, ff), f32),
                pltpu.VMEM((NH, C, rows, d), bf16),
                pltpu.VMEM((NG, C, rows, d), bf16),
                pltpu.VMEM((2 * C, rows, d), bf16),
                pltpu.VMEM((2 * C, rows, d), bf16),
                pltpu.VMEM((C, 2, rows, ff), f32),
                pltpu.VMEM((C, 2, rows, ff), f32),
                pltpu.VMEM((rows, d), bf16),
                pltpu.VMEM((rows, ff), bf16),
                pltpu.VMEM((ND, tokens, ff), bf16),
                pltpu.VMEM((ND, tokens, ff), bf16),
                pltpu.VMEM((ND, tokens, ff), bf16),
                pltpu.VMEM((ND, d, tokens), bf16),
                pltpu.VMEM((ND, d, tokens), bf16),
                dma((3,)),
                dma,
                dma,
                dma((NH * C,)),
                dma((2 * C,)),
                dma((NG * C,)),
                dma((2 * C,)),
                dma((C,)),
                dma((C,)),
                pltpu.SemaphoreType.REGULAR,
                pltpu.SemaphoreType.REGULAR,
            ],
            compiler_params=pltpu.CompilerParams(collective_id=0, has_side_effects=True, vmem_limit_bytes=67043328),
        )(x.reshape(micro, C, rows, d), dy.reshape(micro, C, rows, d), w_gate, w_up, w_down)
        return outs[:3]

    return jax.shard_map(
        step,
        mesh=mesh,
        in_specs=(P("rep", None, None),) * 2 + (P("pp", None, None),) * 3,
        out_specs=(P(("rep", "pp"), None, None),) * 3,
        check_vma=False,
    )
```

```python
import functools

import jax
import jax.numpy as jnp
from jax import lax
from jax.experimental import pallas as pl
from jax.experimental.pallas import tpu as pltpu
from jax.sharding import PartitionSpec as P

Q = 4
COARSE, FINE = 2, 4
FINE_F, FINE_B = 4, 4
NH = 12
NG = 4
ND = 2
TF, TB, TD, TW, TR = 256, 512, 256, 512, 64
EPS = 1e-6


def dot(a, b):
    return jnp.dot(a, b, preferred_element_type=jnp.float32)


def norm(h):
    wide = h.astype(jnp.float32)
    scale = lax.rsqrt(jnp.mean(wide * wide, -1, keepdims=True) + EPS)
    return wide, scale


def kernel(stages, x_hbm, dy_hbm, wg_hbm, wu_hbm, wd_hbm, og_hbm, ou_hbm, od_hbm, spill, acts, wg, wu, wd, wgt, wut, wdt, tg, tu, td, hbuf, gbuf, fsend,
           bsend, keep, back, a_v, act_v, by_a_v, sa, sg, su, at, dt, wsem, xsem, ysem, frecv, fsent, brecv, bsent, keepsem, backsem, fcred, bcred):
    micro, tokens, d = x_hbm.shape
    ff = wg.shape[1]
    part = tokens // Q
    me = lax.axis_index("pp")
    first, last = me == 0, me == stages - 1
    behind = stages - 1 - me
    warm = 1 + lax.div(behind * 4 + 1, 3)
    late = jnp.where(me >= 2, ND - 1, 0)

    loads = [pltpu.make_async_copy(src.at[0], dst, wsem.at[i]) for i, (src, dst) in enumerate(((wg_hbm, wg), (wu_hbm, wu), (wd_hbm, wd)))]
    for load in loads:
        load.start()

    def rows(j, count=1):
        return pl.ds(pl.multiple_of(j * part, part), count * part)

    def x_copy(m):
        return pltpu.make_async_copy(x_hbm.at[m], hbuf.at[lax.rem(m, NH)], xsem)

    def dy_copy(m):
        return pltpu.make_async_copy(dy_hbm.at[m], gbuf.at[lax.rem(m, NG)], ysem)

    @pl.when(first)
    def _():
        x_copy(0).start()

    @pl.when(last)
    def _():
        dy_copy(0).start()

    barrier = pltpu.get_barrier_semaphore()

    @pl.when(me > 0)
    def _():
        pl.semaphore_signal(barrier, inc=1, device_id={"pp": me - 1})

    @pl.when(me < stages - 1)
    def _():
        pl.semaphore_signal(barrier, inc=1, device_id={"pp": me + 1})

    pl.semaphore_wait(barrier, jnp.where(first | last, 1, 2))

    def f_copy(m, j):
        out, slot = lax.rem(m, 2), lax.rem(m, NH)
        return pltpu.make_async_remote_copy(
            src_ref=fsend.at[out, rows(j)], dst_ref=hbuf.at[slot, rows(j)], send_sem=fsent.at[out * Q + j], recv_sem=frecv.at[slot * Q + j],
            device_id={"pp": me + 1},
        )

    def b_copy(m, j):
        out, slot = lax.rem(m, 2), lax.rem(m, NG)
        return pltpu.make_async_remote_copy(
            src_ref=bsend.at[out, rows(j)], dst_ref=gbuf.at[slot, rows(j)], send_sem=bsent.at[out * Q + j], recv_sem=brecv.at[slot * Q + j],
            device_id={"pp": me - 1},
        )

    def keep_copy(m, j):
        return pltpu.make_async_copy(keep.at[:, rows(j)], spill.at[m, :, rows(j)], keepsem.at[j])

    def act_copy(m, j):
        return pltpu.make_async_copy(act_v.at[rows(j)], acts.at[m, rows(j)], keepsem.at[Q + j])

    def back_copy(m, j):
        return pltpu.make_async_copy(spill.at[m, :, rows(j)], back.at[:, rows(j)], backsem.at[j])

    def sa_copy(m):
        return pltpu.make_async_copy(acts.at[m], sa, backsem.at[Q])

    for load in loads:
        load.wait()

    def forward(m, blocks):
        slot, out, each = lax.rem(m, NH), lax.rem(m, 2), Q // blocks

        def hidden(r):
            wide, scale = norm(hbuf[slot, r])
            a = (wide * scale).astype(jnp.bfloat16)
            a_v[r, :] = a
            for n in range(0, ff, TF):
                n = slice(n, n + TF)
                gate, up = dot(a_v[r, :], wg[:, n]), dot(a_v[r, :], wu[:, n])
                s = jax.nn.sigmoid(gate)
                silu = gate * s
                keep[0, r, n] = silu
                keep[1, r, n] = up * (s + silu * (1.0 - s))
                act_v[r, n] = (silu * up).astype(jnp.bfloat16)

        def block(i, _):
            r = rows(i * each, each)
            for j in range(each):
                @pl.when(me > 0)
                def _():
                    f_copy(m, i * each + j).wait_recv()

                @pl.when((me < stages - 1) & (m >= 2))
                def _():
                    f_copy(m - 2, i * each + j).wait_send()

            @pl.when(last)
            def _():
                hidden(r)

            @pl.when(me < stages - 1)
            def _():
                hidden(r)
                for n in range(0, d, TD):
                    n = slice(n, min(n + TD, d))
                    fsend[out, r, n] = hbuf[slot, r, n] + dot(act_v[r, :], wd[:, n]).astype(jnp.bfloat16)
                for j in range(each):
                    f_copy(m, i * each + j).start()

            for j in range(each):
                keep_copy(m, i * each + j).start()
                act_copy(m, i * each + j).start()

            return 0

        lax.fori_loop(0, blocks, block, 0)

    def forwards(m):
        @pl.when(first)
        def _():
            x_copy(m).wait()

            @pl.when(m + 1 < micro)
            def _():
                x_copy(m + 1).start()

        @pl.when((me < stages - 1) & (m >= NH))
        def _():
            pl.semaphore_wait(fcred, 1)

        @pl.when(m < FINE_F)
        def _():
            forward(m, FINE)

        @pl.when(m >= FINE_F)
        def _():
            forward(m, COARSE)

    def backward(m, blocks):
        slot, hslot, q, out, each = lax.rem(m, NG), lax.rem(m, NH), lax.rem(m, ND), lax.rem(m, 2), Q // blocks

        def hidden(r):
            for n in range(0, ff, TB):
                n = slice(n, n + TB)
                by_act = dot(gbuf[slot, r], wdt[:, n]).astype(jnp.bfloat16).astype(jnp.float32)
                su[q, r, n] = (by_act * back[0, r, n]).astype(jnp.bfloat16)
                sg[q, r, n] = (by_act * back[1, r, n]).astype(jnp.bfloat16)
            wide, scale = norm(hbuf[hslot, r])
            at[q, :, r] = (wide * scale).astype(jnp.bfloat16).T
            dt[q, :, r] = gbuf[slot, r].T

        def block(i, _):
            r = rows(i * each, each)
            for j in range(each):
                @pl.when(me < stages - 1)
                def _():
                    b_copy(m, i * each + j).wait_recv()

                @pl.when((me > 0) & (m >= 2))
                def _():
                    b_copy(m - 2, i * each + j).wait_send()

                back_copy(m, i * each + j).wait()

            @pl.when(first)
            def _():
                hidden(r)

            @pl.when(me > 0)
            def _():
                hidden(r)
                for n in range(0, d, TD):
                    n = slice(n, min(n + TD, d))
                    by_a_v[0 : each * part, n] = dot(sg[q, r, :], wgt[:, n]).astype(jnp.bfloat16) + dot(su[q, r, :], wut[:, n]).astype(jnp.bfloat16)
                for p in range(0, each * part, TR):
                    o = pl.ds(pl.multiple_of(i * each * part + p, TR), TR)
                    by_a = by_a_v[p : p + TR, :].astype(jnp.float32)
                    wide, scale = norm(hbuf[hslot, o])
                    by_scale = jnp.sum(by_a * wide, -1, keepdims=True)
                    by_wide = by_a * scale - wide * (by_scale * (scale * scale * scale) * (1.0 / d))
                    bsend[out, o] = by_wide.astype(jnp.bfloat16) + gbuf[slot, o]
                for j in range(each):
                    b_copy(m, i * each + j).start()

            return 0

        lax.fori_loop(0, blocks, block, 0)

    def backwards(m):
        @pl.when(last)
        def _():
            dy_copy(m).wait()

            @pl.when(m + 1 < micro)
            def _():
                dy_copy(m + 1).start()

        @pl.when((me > 0) & (m >= NG))
        def _():
            pl.semaphore_wait(bcred, 1)

        @pl.when(m < micro - FINE_B)
        def _():
            backward(m, COARSE)

        @pl.when(m >= micro - FINE_B)
        def _():
            backward(m, FINE)

        @pl.when((me > 0) & (m + NH < micro))
        def _():
            pl.semaphore_signal(fcred, inc=1, device_id={"pp": me - 1})

        @pl.when((me < stages - 1) & (m + NG < micro))
        def _():
            pl.semaphore_signal(bcred, inc=1, device_id={"pp": me + 1})

    def term(total, left, right):
        for n in range(0, ff, TW):
            n = slice(n, n + TW)
            total[:, n] += dot(left[...], right[:, n]).astype(jnp.bfloat16).astype(jnp.float32)

    def step(t, _):
        f, b = t, t - warm
        w = b - late
        q = lax.rem(w + ND * micro, ND)
        f_on, w_on, more = f < micro, (w >= 0) & (w < micro), (b + 1 >= 0) & (b + 1 < micro)

        @pl.when((b >= 0) & (b < micro))
        def _():
            backwards(b)

        @pl.when(more & (warm > 1))
        def _():
            for j in range(Q):
                back_copy(b + 1, j).start()

        @pl.when(f_on)
        def _():
            forwards(f)

        @pl.when(w_on)
        def _():
            term(tg, at.at[q], sg.at[q])

        @pl.when(f_on)
        def _():
            for j in range(Q):
                keep_copy(f, j).wait()
                act_copy(f, j).wait()

        @pl.when(more & (warm == 1))
        def _():
            for j in range(Q):
                back_copy(b + 1, j).start()

        @pl.when(w_on)
        def _():
            term(tu, at.at[q], su.at[q])
            sa_copy(w).wait()
            term(td, dt.at[q], sa)

        @pl.when((w + 1 >= 0) & (w + 1 < micro))
        def _():
            sa_copy(w + 1).start()

        return 0

    wgt[...] = wg[...].T
    wut[...] = wu[...].T
    wdt[...] = wd[...].T
    for total in (tg, tu, td):
        total[...] = jnp.zeros_like(total)

    lax.fori_loop(0, micro + warm + late, step, 0)

    for m in (micro - 2, micro - 1):
        for j in range(Q):
            @pl.when(me < stages - 1)
            def _():
                f_copy(m, j).wait_send()

            @pl.when(me > 0)
            def _():
                b_copy(m, j).wait_send()

    wg[...] = tg[...].astype(jnp.bfloat16)
    wu[...] = tu[...].astype(jnp.bfloat16)
    wd[...] = td[...].astype(jnp.bfloat16).T
    stores = [pltpu.make_async_copy(src, dst.at[0], wsem.at[i]) for i, (src, dst) in enumerate(((wg, og_hbm), (wu, ou_hbm), (wd, od_hbm)))]
    for store in stores:
        store.start()
    for store in stores:
        store.wait()


def solution(mesh):
    stages = mesh.shape["pp"]

    def step(x, dy, w_gate, w_up, w_down):
        micro, tokens, d = x.shape
        ff = w_gate.shape[2]
        bf16, f32 = jnp.bfloat16, jnp.float32
        anywhere = pl.BlockSpec(memory_space=pl.ANY)
        dma = pltpu.SemaphoreType.DMA
        outs = pl.pallas_call(
            functools.partial(kernel, stages),
            out_shape=(
                jax.ShapeDtypeStruct(w_gate.shape, bf16),
                jax.ShapeDtypeStruct(w_up.shape, bf16),
                jax.ShapeDtypeStruct(w_down.shape, bf16),
                jax.ShapeDtypeStruct((micro, 2, tokens, ff), f32),
                jax.ShapeDtypeStruct((micro, tokens, ff), bf16),
            ),
            in_specs=[anywhere] * 5,
            out_specs=(anywhere,) * 5,
            scratch_shapes=[
                pltpu.VMEM((d, ff), bf16),
                pltpu.VMEM((d, ff), bf16),
                pltpu.VMEM((ff, d), bf16),
                pltpu.VMEM((ff, d), bf16),
                pltpu.VMEM((ff, d), bf16),
                pltpu.VMEM((d, ff), bf16),
                pltpu.VMEM((d, ff), f32),
                pltpu.VMEM((d, ff), f32),
                pltpu.VMEM((d, ff), f32),
                pltpu.VMEM((NH, tokens, d), bf16),
                pltpu.VMEM((NG, tokens, d), bf16),
                pltpu.VMEM((2, tokens, d), bf16),
                pltpu.VMEM((2, tokens, d), bf16),
                pltpu.VMEM((2, tokens, ff), f32),
                pltpu.VMEM((2, tokens, ff), f32),
                pltpu.VMEM((tokens, d), bf16),
                pltpu.VMEM((tokens, ff), bf16),
                pltpu.VMEM((tokens // COARSE, d), bf16),
                pltpu.VMEM((tokens, ff), bf16),
                pltpu.VMEM((ND, tokens, ff), bf16),
                pltpu.VMEM((ND, tokens, ff), bf16),
                pltpu.VMEM((ND, d, tokens), bf16),
                pltpu.VMEM((ND, d, tokens), bf16),
                dma((3,)),
                dma,
                dma,
                dma((NH * Q,)),
                dma((2 * Q,)),
                dma((NG * Q,)),
                dma((2 * Q,)),
                dma((2 * Q,)),
                dma((Q + 1,)),
                pltpu.SemaphoreType.REGULAR,
                pltpu.SemaphoreType.REGULAR,
            ],
            compiler_params=pltpu.CompilerParams(collective_id=0, has_side_effects=True, vmem_limit_bytes=67043328),
        )(x, dy, w_gate, w_up, w_down)
        return outs[:3]

    return jax.shard_map(
        step,
        mesh=mesh,
        in_specs=(P("rep", None, None),) * 2 + (P("pp", None, None),) * 3,
        out_specs=(P(("rep", "pp"), None, None),) * 3,
        check_vma=False,
    )
```

```python
import functools

import jax
import jax.numpy as jnp
from jax import lax
from jax.experimental import pallas as pl
from jax.experimental.pallas import tpu as pltpu
from jax.sharding import PartitionSpec as P

Q = 4
COARSE, FINE = 2, 4
FINE_F, FINE_B = 5, 5
NH = 14
NG = 3
ND = 2
TF, TB, TD, TW, TR = 256, 512, 256, 512, 64
EPS = 1e-6


def dot(a, b):
    return jnp.dot(a, b, preferred_element_type=jnp.float32)


def dot_t(a, b):
    return lax.dot_general(a, b, (((1,), (1,)), ((), ())), preferred_element_type=jnp.float32)


def norm(h):
    wide = h.astype(jnp.float32)
    scale = lax.rsqrt(jnp.mean(wide * wide, -1, keepdims=True) + EPS)
    return wide, scale


def kernel(stages, x_hbm, dy_hbm, wg_hbm, wu_hbm, wd_hbm, og_hbm, ou_hbm, od_hbm, spill, acts, wg, wu, wd, wgt, wut, wdt, tg, tu, td, hbuf, gbuf, fsend,
           bsend, keep, back, a_v, act_v, by_a_v, sa, sg, su, at, dt, wsem, xsem, ysem, frecv, fsent, brecv, bsent, keepsem, backsem, fcred, bcred):
    micro, tokens, d = x_hbm.shape
    ff = wg.shape[1]
    part = tokens // Q
    me = lax.axis_index("pp")
    first, last = me == 0, me == stages - 1
    behind = stages - 1 - me
    warm = jnp.minimum(1 + lax.div(behind * 3, 2) + jnp.where(me < 2, 4, 0), NH - 1)
    late = jnp.clip(me - 2, 0, ND - 1)

    loads = [pltpu.make_async_copy(src.at[0], dst, wsem.at[i]) for i, (src, dst) in enumerate(((wg_hbm, wg), (wu_hbm, wu), (wd_hbm, wd)))]
    for load in loads:
        load.start()

    def rows(j, count=1):
        return pl.ds(pl.multiple_of(j * part, part), count * part)

    def x_copy(m):
        return pltpu.make_async_copy(x_hbm.at[m], hbuf.at[lax.rem(m, NH)], xsem)

    def dy_copy(m):
        return pltpu.make_async_copy(dy_hbm.at[m], gbuf.at[lax.rem(m, NG)], ysem)

    @pl.when(first)
    def _():
        x_copy(0).start()

    @pl.when(last)
    def _():
        dy_copy(0).start()

    barrier = pltpu.get_barrier_semaphore()

    @pl.when(me > 0)
    def _():
        pl.semaphore_signal(barrier, inc=1, device_id={"pp": me - 1})

    @pl.when(me < stages - 1)
    def _():
        pl.semaphore_signal(barrier, inc=1, device_id={"pp": me + 1})

    pl.semaphore_wait(barrier, jnp.where(first | last, 1, 2))

    def f_copy(m, j):
        out, slot = lax.rem(m, 2), lax.rem(m, NH)
        return pltpu.make_async_remote_copy(
            src_ref=fsend.at[out, rows(j)], dst_ref=hbuf.at[slot, rows(j)], send_sem=fsent.at[out * Q + j], recv_sem=frecv.at[slot * Q + j],
            device_id={"pp": me + 1},
        )

    def b_copy(m, j):
        out, slot = lax.rem(m, 2), lax.rem(m, NG)
        return pltpu.make_async_remote_copy(
            src_ref=bsend.at[out, rows(j)], dst_ref=gbuf.at[slot, rows(j)], send_sem=bsent.at[out * Q + j], recv_sem=brecv.at[slot * Q + j],
            device_id={"pp": me - 1},
        )

    def keep_copy(m, j):
        return pltpu.make_async_copy(keep.at[:, rows(j)], spill.at[m, :, rows(j)], keepsem.at[j])

    def act_copy(m, j):
        return pltpu.make_async_copy(act_v.at[rows(j)], acts.at[m, rows(j)], keepsem.at[Q + j])

    def back_copy(m, j):
        return pltpu.make_async_copy(spill.at[m, :, rows(j)], back.at[:, rows(j)], backsem.at[j])

    def sa_copy(m):
        return pltpu.make_async_copy(acts.at[m], sa, backsem.at[Q])

    for load in loads:
        load.wait()

    def forward(m, blocks):
        slot, out, each = lax.rem(m, NH), lax.rem(m, 2), Q // blocks

        def hidden(r):
            wide, scale = norm(hbuf[slot, r])
            a = (wide * scale).astype(jnp.bfloat16)
            a_v[r, :] = a
            for n in range(0, ff, TF):
                n = slice(n, n + TF)
                gate, up = dot(a_v[r, :], wg[:, n]), dot(a_v[r, :], wu[:, n])
                s = jax.nn.sigmoid(gate)
                silu = gate * s
                keep[0, r, n] = silu
                keep[1, r, n] = up * (s + silu * (1.0 - s))
                act_v[r, n] = (silu * up).astype(jnp.bfloat16)

        def block(i, _):
            r = rows(i * each, each)
            for j in range(each):
                @pl.when(me > 0)
                def _():
                    f_copy(m, i * each + j).wait_recv()

                @pl.when((me < stages - 1) & (m >= 2))
                def _():
                    f_copy(m - 2, i * each + j).wait_send()

            @pl.when(last)
            def _():
                hidden(r)

            @pl.when(me < stages - 1)
            def _():
                hidden(r)
                if blocks == COARSE:
                    fsend[out, r] = hbuf[slot, r] + dot_t(wdt[...], act_v[r, :]).astype(jnp.bfloat16).T
                else:
                    for n in range(0, d, TD):
                        n = slice(n, min(n + TD, d))
                        fsend[out, r, n] = hbuf[slot, r, n] + dot(act_v[r, :], wd[:, n]).astype(jnp.bfloat16)
                for j in range(each):
                    f_copy(m, i * each + j).start()

            for j in range(each):
                keep_copy(m, i * each + j).start()
                act_copy(m, i * each + j).start()

            return 0

        lax.fori_loop(0, blocks, block, 0)

    def forwards(m):
        @pl.when(first)
        def _():
            x_copy(m).wait()

            @pl.when(m + 1 < micro)
            def _():
                x_copy(m + 1).start()

        @pl.when((me < stages - 1) & (m >= NH))
        def _():
            pl.semaphore_wait(fcred, 1)

        @pl.when(m < FINE_F)
        def _():
            forward(m, FINE)

        @pl.when(m >= FINE_F)
        def _():
            forward(m, COARSE)

    def backward(m, blocks):
        slot, hslot, q, out, each = lax.rem(m, NG), lax.rem(m, NH), lax.rem(m, ND), lax.rem(m, 2), Q // blocks

        def hidden(r):
            for n in range(0, ff, TB):
                n = slice(n, n + TB)
                by_act = dot(gbuf[slot, r], wdt[:, n]).astype(jnp.bfloat16).astype(jnp.float32)
                su[q, r, n] = (by_act * back[0, r, n]).astype(jnp.bfloat16)
                sg[q, r, n] = (by_act * back[1, r, n]).astype(jnp.bfloat16)
            wide, scale = norm(hbuf[hslot, r])
            at[q, :, r] = (wide * scale).astype(jnp.bfloat16).T
            dt[q, :, r] = gbuf[slot, r].T

        def block(i, _):
            r = rows(i * each, each)
            for j in range(each):
                @pl.when(me < stages - 1)
                def _():
                    b_copy(m, i * each + j).wait_recv()

                @pl.when((me > 0) & (m >= 2))
                def _():
                    b_copy(m - 2, i * each + j).wait_send()

                back_copy(m, i * each + j).wait()

            @pl.when(first)
            def _():
                hidden(r)

            @pl.when(me > 0)
            def _():
                hidden(r)
                if blocks == COARSE:
                    by_at = dot_t(wg[...], sg[q, r, :]).astype(jnp.bfloat16) + dot_t(wu[...], su[q, r, :]).astype(jnp.bfloat16)
                    by_a_v[...] = by_at.T
                else:
                    for n in range(0, d, TD):
                        n = slice(n, min(n + TD, d))
                        by_a = dot(sg[q, r, :], wgt[:, n]).astype(jnp.bfloat16) + dot(su[q, r, :], wut[:, n]).astype(jnp.bfloat16)
                        by_a_v[0 : each * part, n] = by_a
                for p in range(0, each * part, TR):
                    o = pl.ds(pl.multiple_of(i * each * part + p, TR), TR)
                    by_a = by_a_v[p : p + TR, :].astype(jnp.float32)
                    wide, scale = norm(hbuf[hslot, o])
                    by_scale = jnp.sum(by_a * wide, -1, keepdims=True)
                    by_wide = by_a * scale - wide * (by_scale * (scale * scale * scale) * (1.0 / d))
                    bsend[out, o] = by_wide.astype(jnp.bfloat16) + gbuf[slot, o]
                for j in range(each):
                    b_copy(m, i * each + j).start()

            return 0

        lax.fori_loop(0, blocks, block, 0)

    def backwards(m):
        @pl.when(last)
        def _():
            dy_copy(m).wait()

            @pl.when(m + 1 < micro)
            def _():
                dy_copy(m + 1).start()

        @pl.when((me > 0) & (m >= NG))
        def _():
            pl.semaphore_wait(bcred, 1)

        @pl.when(m < micro - FINE_B)
        def _():
            backward(m, COARSE)

        @pl.when(m >= micro - FINE_B)
        def _():
            backward(m, FINE)

        @pl.when((me > 0) & (m + NH < micro))
        def _():
            pl.semaphore_signal(fcred, inc=1, device_id={"pp": me - 1})

        @pl.when((me < stages - 1) & (m + NG < micro))
        def _():
            pl.semaphore_signal(bcred, inc=1, device_id={"pp": me + 1})

    def term(total, left, right):
        for n in range(0, ff, TW):
            n = slice(n, n + TW)
            total[:, n] += dot(left[...], right[:, n]).astype(jnp.bfloat16).astype(jnp.float32)

    def step(t, _):
        f, b = t, t - warm
        w = b - late
        q = lax.rem(w + ND * micro, ND)
        f_on, w_on, more = f < micro, (w >= 0) & (w < micro), (b + 1 >= 0) & (b + 1 < micro)

        @pl.when((b >= 0) & (b < micro))
        def _():
            backwards(b)

        @pl.when(more & (warm > 1))
        def _():
            for j in range(Q):
                back_copy(b + 1, j).start()

        @pl.when(f_on)
        def _():
            forwards(f)

        @pl.when(t == 0)
        def _():
            for total in (tg, tu, td):
                total[...] = jnp.zeros_like(total)
            wgt[...] = wg[...].T
            wut[...] = wu[...].T
            wdt[...] = wd[...].T

        @pl.when(w_on)
        def _():
            term(tg, at.at[q], sg.at[q])

        @pl.when(f_on & (warm == 1))
        def _():
            for j in range(Q):
                keep_copy(f, j).wait()
                act_copy(f, j).wait()

        @pl.when(more & (warm == 1))
        def _():
            for j in range(Q):
                back_copy(b + 1, j).start()

        @pl.when(w_on)
        def _():
            term(tu, at.at[q], su.at[q])
            sa_copy(w).wait()
            term(td, dt.at[q], sa)

        @pl.when(f_on & (warm > 1))
        def _():
            for j in range(Q):
                keep_copy(f, j).wait()
                act_copy(f, j).wait()

        @pl.when((w + 1 >= 0) & (w + 1 < micro))
        def _():
            sa_copy(w + 1).start()

        return 0

    lax.fori_loop(0, micro + warm + late, step, 0)

    for m in (micro - 2, micro - 1):
        for j in range(Q):
            @pl.when(me < stages - 1)
            def _():
                f_copy(m, j).wait_send()

            @pl.when(me > 0)
            def _():
                b_copy(m, j).wait_send()

    stores = [pltpu.make_async_copy(src, dst.at[0], wsem.at[i]) for i, (src, dst) in enumerate(((wg, og_hbm), (wu, ou_hbm), (wd, od_hbm)))]
    wg[...] = tg[...].astype(jnp.bfloat16)
    stores[0].start()
    wu[...] = tu[...].astype(jnp.bfloat16)
    stores[1].start()
    wd[...] = td[...].astype(jnp.bfloat16).T
    stores[2].start()
    for store in stores:
        store.wait()


def solution(mesh):
    stages = mesh.shape["pp"]

    def step(x, dy, w_gate, w_up, w_down):
        micro, tokens, d = x.shape
        ff = w_gate.shape[2]
        bf16, f32 = jnp.bfloat16, jnp.float32
        anywhere = pl.BlockSpec(memory_space=pl.ANY)
        dma = pltpu.SemaphoreType.DMA
        outs = pl.pallas_call(
            functools.partial(kernel, stages),
            out_shape=(
                jax.ShapeDtypeStruct(w_gate.shape, bf16),
                jax.ShapeDtypeStruct(w_up.shape, bf16),
                jax.ShapeDtypeStruct(w_down.shape, bf16),
                jax.ShapeDtypeStruct((micro, 2, tokens, ff), f32),
                jax.ShapeDtypeStruct((micro, tokens, ff), bf16),
            ),
            in_specs=[anywhere] * 5,
            out_specs=(anywhere,) * 5,
            scratch_shapes=[
                pltpu.VMEM((d, ff), bf16),
                pltpu.VMEM((d, ff), bf16),
                pltpu.VMEM((ff, d), bf16),
                pltpu.VMEM((ff, d), bf16),
                pltpu.VMEM((ff, d), bf16),
                pltpu.VMEM((d, ff), bf16),
                pltpu.VMEM((d, ff), f32),
                pltpu.VMEM((d, ff), f32),
                pltpu.VMEM((d, ff), f32),
                pltpu.VMEM((NH, tokens, d), bf16),
                pltpu.VMEM((NG, tokens, d), bf16),
                pltpu.VMEM((2, tokens, d), bf16),
                pltpu.VMEM((2, tokens, d), bf16),
                pltpu.VMEM((2, tokens, ff), f32),
                pltpu.VMEM((2, tokens, ff), f32),
                pltpu.VMEM((tokens, d), bf16),
                pltpu.VMEM((tokens, ff), bf16),
                pltpu.VMEM((tokens // COARSE, d), bf16),
                pltpu.VMEM((tokens, ff), bf16),
                pltpu.VMEM((ND, tokens, ff), bf16),
                pltpu.VMEM((ND, tokens, ff), bf16),
                pltpu.VMEM((ND, d, tokens), bf16),
                pltpu.VMEM((ND, d, tokens), bf16),
                dma((3,)),
                dma,
                dma,
                dma((NH * Q,)),
                dma((2 * Q,)),
                dma((NG * Q,)),
                dma((2 * Q,)),
                dma((2 * Q,)),
                dma((Q + 1,)),
                pltpu.SemaphoreType.REGULAR,
                pltpu.SemaphoreType.REGULAR,
            ],
            compiler_params=pltpu.CompilerParams(collective_id=0, has_side_effects=True, vmem_limit_bytes=67043328),
        )(x, dy, w_gate, w_up, w_down)
        return outs[:3]

    return jax.shard_map(
        step,
        mesh=mesh,
        in_specs=(P("rep", None, None),) * 2 + (P("pp", None, None),) * 3,
        out_specs=(P(("rep", "pp"), None, None),) * 3,
        check_vma=False,
    )
```

```python
import functools

import jax
import jax.numpy as jnp
from jax import lax
from jax.experimental import pallas as pl
from jax.experimental.pallas import tpu as pltpu
from jax.sharding import PartitionSpec as P

Q = 4
COARSE, FINE = 2, 4
FINE_F, FINE_B = 5, 5
NH = 14
NG = 3
ND = 2
TF, TB, TD, TW, TR = 256, 512, 256, 512, 64
EPS = 1e-6


def dot(a, b):
    return jnp.dot(a, b, preferred_element_type=jnp.float32)


def dot_t(a, b):
    return lax.dot_general(a, b, (((1,), (1,)), ((), ())), preferred_element_type=jnp.float32)


def norm(h):
    wide = h.astype(jnp.float32)
    scale = lax.rsqrt(jnp.mean(wide * wide, -1, keepdims=True) + EPS)
    return wide, scale


def kernel(stages, x_hbm, dy_hbm, wg_hbm, wu_hbm, wd_hbm, og_hbm, ou_hbm, od_hbm, spill, acts, wg, wu, wd, wgt, wut, wdt, tg, tu, td, hbuf, gbuf, fsend,
           bsend, pool, a_v, act_v, by_a_v, sa, sg, su, at, dt, wsem, xsem, ysem, frecv, fsent, brecv, bsent, keepsem, backsem, fcred, bcred):
    micro, tokens, d = x_hbm.shape
    ff = wg.shape[1]
    part = tokens // Q
    me = lax.axis_index("pp")
    first, last = me == 0, me == stages - 1
    behind = stages - 1 - me
    warm = jnp.minimum(1 + lax.div(behind * 3, 2) + jnp.where(me < 2, 4, 0), NH - 1)
    late = jnp.clip(me - 2, 0, ND - 1)
    resident = warm <= 2

    loads = [pltpu.make_async_copy(src.at[0], dst, wsem.at[i]) for i, (src, dst) in enumerate(((wg_hbm, wg), (wu_hbm, wu), (wd_hbm, wd)))]
    for load in loads:
        load.start()

    def rows(j, count=1):
        return pl.ds(pl.multiple_of(j * part, part), count * part)

    def x_copy(m):
        return pltpu.make_async_copy(x_hbm.at[m], hbuf.at[lax.rem(m, NH)], xsem)

    def dy_copy(m):
        return pltpu.make_async_copy(dy_hbm.at[m], gbuf.at[lax.rem(m, NG)], ysem)

    @pl.when(first)
    def _():
        x_copy(0).start()

    @pl.when(last)
    def _():
        dy_copy(0).start()

    barrier = pltpu.get_barrier_semaphore()

    @pl.when(me > 0)
    def _():
        pl.semaphore_signal(barrier, inc=1, device_id={"pp": me - 1})

    @pl.when(me < stages - 1)
    def _():
        pl.semaphore_signal(barrier, inc=1, device_id={"pp": me + 1})

    pl.semaphore_wait(barrier, jnp.where(first | last, 1, 2))

    def f_copy(m, j):
        out, slot = lax.rem(m, 2), lax.rem(m, NH)
        return pltpu.make_async_remote_copy(
            src_ref=fsend.at[out, rows(j)], dst_ref=hbuf.at[slot, rows(j)], send_sem=fsent.at[out * Q + j], recv_sem=frecv.at[slot * Q + j],
            device_id={"pp": me + 1},
        )

    def b_copy(m, j):
        out, slot = lax.rem(m, 2), lax.rem(m, NG)
        return pltpu.make_async_remote_copy(
            src_ref=bsend.at[out, rows(j)], dst_ref=gbuf.at[slot, rows(j)], send_sem=bsent.at[out * Q + j], recv_sem=brecv.at[slot * Q + j],
            device_id={"pp": me - 1},
        )

    def keep_copy(m, j):
        return pltpu.make_async_copy(pool.at[0, :, rows(j)], spill.at[m, :, rows(j)], keepsem.at[j])

    def act_copy(m, j):
        return pltpu.make_async_copy(act_v.at[rows(j)], acts.at[m, rows(j)], keepsem.at[Q + j])

    def back_copy(m, j):
        return pltpu.make_async_copy(spill.at[m, :, rows(j)], pool.at[1, :, rows(j)], backsem.at[j])

    def sa_copy(m):
        return pltpu.make_async_copy(acts.at[m], sa, backsem.at[Q])

    for load in loads:
        load.wait()

    def forward(m, blocks):
        slot, out, each = lax.rem(m, NH), lax.rem(m, 2), Q // blocks
        place = jnp.where(resident, lax.rem(m, 2), 0)

        def hidden(r):
            wide, scale = norm(hbuf[slot, r])
            a = (wide * scale).astype(jnp.bfloat16)
            a_v[r, :] = a
            for n in range(0, ff, TF):
                n = slice(n, n + TF)
                gate, up = dot(a_v[r, :], wg[:, n]), dot(a_v[r, :], wu[:, n])
                s = jax.nn.sigmoid(gate)
                silu = gate * s
                pool[place, 0, r, n] = silu
                pool[place, 1, r, n] = up * (s + silu * (1.0 - s))
                act_v[r, n] = (silu * up).astype(jnp.bfloat16)

        def block(i, _):
            r = rows(i * each, each)
            for j in range(each):
                @pl.when(me > 0)
                def _():
                    f_copy(m, i * each + j).wait_recv()

                @pl.when((me < stages - 1) & (m >= 2))
                def _():
                    f_copy(m - 2, i * each + j).wait_send()

            @pl.when(last)
            def _():
                hidden(r)

            @pl.when(me < stages - 1)
            def _():
                hidden(r)
                if blocks == COARSE:
                    fsend[out, r] = hbuf[slot, r] + dot_t(wdt[...], act_v[r, :]).astype(jnp.bfloat16).T
                else:
                    for n in range(0, d, TD):
                        n = slice(n, min(n + TD, d))
                        fsend[out, r, n] = hbuf[slot, r, n] + dot(act_v[r, :], wd[:, n]).astype(jnp.bfloat16)
                for j in range(each):
                    f_copy(m, i * each + j).start()

            for j in range(each):
                act_copy(m, i * each + j).start()

                @pl.when(jnp.logical_not(resident))
                def _():
                    keep_copy(m, i * each + j).start()

            return 0

        lax.fori_loop(0, blocks, block, 0)

    def forwards(m):
        @pl.when(first)
        def _():
            x_copy(m).wait()

            @pl.when(m + 1 < micro)
            def _():
                x_copy(m + 1).start()

        @pl.when((me < stages - 1) & (m >= NH))
        def _():
            pl.semaphore_wait(fcred, 1)

        @pl.when(m < FINE_F)
        def _():
            forward(m, FINE)

        @pl.when(m >= FINE_F)
        def _():
            forward(m, COARSE)

    def backward(m, blocks):
        slot, hslot, q, out, each = lax.rem(m, NG), lax.rem(m, NH), lax.rem(m, ND), lax.rem(m, 2), Q // blocks
        place = jnp.where(resident, lax.rem(m, 2), 1)

        def hidden(r):
            for n in range(0, ff, TB):
                n = slice(n, n + TB)
                by_act = dot(gbuf[slot, r], wdt[:, n]).astype(jnp.bfloat16).astype(jnp.float32)
                su[q, r, n] = (by_act * pool[place, 0, r, n]).astype(jnp.bfloat16)
                sg[q, r, n] = (by_act * pool[place, 1, r, n]).astype(jnp.bfloat16)
            wide, scale = norm(hbuf[hslot, r])
            at[q, :, r] = (wide * scale).astype(jnp.bfloat16).T
            dt[q, :, r] = gbuf[slot, r].T

        def block(i, _):
            r = rows(i * each, each)
            for j in range(each):
                @pl.when(me < stages - 1)
                def _():
                    b_copy(m, i * each + j).wait_recv()

                @pl.when((me > 0) & (m >= 2))
                def _():
                    b_copy(m - 2, i * each + j).wait_send()

                @pl.when(jnp.logical_not(resident))
                def _():
                    back_copy(m, i * each + j).wait()

            @pl.when(first)
            def _():
                hidden(r)

            @pl.when(me > 0)
            def _():
                hidden(r)
                if blocks == COARSE:
                    by_at = dot_t(wg[...], sg[q, r, :]).astype(jnp.bfloat16) + dot_t(wu[...], su[q, r, :]).astype(jnp.bfloat16)
                    by_a_v[...] = by_at.T
                else:
                    for n in range(0, d, TD):
                        n = slice(n, min(n + TD, d))
                        by_a = dot(sg[q, r, :], wgt[:, n]).astype(jnp.bfloat16) + dot(su[q, r, :], wut[:, n]).astype(jnp.bfloat16)
                        by_a_v[0 : each * part, n] = by_a
                for p in range(0, each * part, TR):
                    o = pl.ds(pl.multiple_of(i * each * part + p, TR), TR)
                    by_a = by_a_v[p : p + TR, :].astype(jnp.float32)
                    wide, scale = norm(hbuf[hslot, o])
                    by_scale = jnp.sum(by_a * wide, -1, keepdims=True)
                    by_wide = by_a * scale - wide * (by_scale * (scale * scale * scale) * (1.0 / d))
                    bsend[out, o] = by_wide.astype(jnp.bfloat16) + gbuf[slot, o]
                for j in range(each):
                    b_copy(m, i * each + j).start()

            return 0

        lax.fori_loop(0, blocks, block, 0)

    def backwards(m):
        @pl.when(last)
        def _():
            dy_copy(m).wait()

            @pl.when(m + 1 < micro)
            def _():
                dy_copy(m + 1).start()

        @pl.when((me > 0) & (m >= NG))
        def _():
            pl.semaphore_wait(bcred, 1)

        @pl.when(m < micro - FINE_B)
        def _():
            backward(m, COARSE)

        @pl.when(m >= micro - FINE_B)
        def _():
            backward(m, FINE)

        @pl.when((me > 0) & (m + NH < micro))
        def _():
            pl.semaphore_signal(fcred, inc=1, device_id={"pp": me - 1})

        @pl.when((me < stages - 1) & (m + NG < micro))
        def _():
            pl.semaphore_signal(bcred, inc=1, device_id={"pp": me + 1})

    def term(total, left, right):
        for n in range(0, ff, TW):
            n = slice(n, n + TW)
            total[:, n] += dot(left[...], right[:, n]).astype(jnp.bfloat16).astype(jnp.float32)

    stores = [pltpu.make_async_copy(src, dst.at[0], wsem.at[i]) for i, (src, dst) in enumerate(((wg, og_hbm), (wu, ou_hbm), (wd, od_hbm)))]

    def step(t, _):
        f, b = t, t - warm
        w = b - late
        q = lax.rem(w + ND * micro, ND)
        f_on, w_on, more = f < micro, (w >= 0) & (w < micro), (b + 1 >= 0) & (b + 1 < micro)

        @pl.when((b >= 0) & (b < micro))
        def _():
            backwards(b)

        @pl.when(more & jnp.logical_not(resident))
        def _():
            for j in range(Q):
                back_copy(b + 1, j).start()

        @pl.when(f_on)
        def _():
            forwards(f)

        @pl.when(t == 0)
        def _():
            for total in (tg, tu, td):
                total[...] = jnp.zeros_like(total)
            wgt[...] = wg[...].T
            wut[...] = wu[...].T
            wdt[...] = wd[...].T

        @pl.when(w_on)
        def _():
            sa_copy(w).wait()

        @pl.when(w_on & (w < micro - 1))
        def _():
            term(tg, at.at[q], sg.at[q])
            term(tu, at.at[q], su.at[q])
            term(td, dt.at[q], sa)

        @pl.when(w == micro - 1)
        def _():
            term(tg, at.at[q], sg.at[q])
            wg[...] = tg[...].astype(jnp.bfloat16)
            stores[0].start()
            term(tu, at.at[q], su.at[q])
            wu[...] = tu[...].astype(jnp.bfloat16)
            stores[1].start()
            term(td, dt.at[q], sa)
            wd[...] = td[...].astype(jnp.bfloat16).T
            stores[2].start()

        @pl.when(f_on)
        def _():
            for j in range(Q):
                act_copy(f, j).wait()

                @pl.when(jnp.logical_not(resident))
                def _():
                    keep_copy(f, j).wait()

        @pl.when((w + 1 >= 0) & (w + 1 < micro))
        def _():
            sa_copy(w + 1).start()

        return 0

    lax.fori_loop(0, micro + warm + late, step, 0)

    for m in (micro - 2, micro - 1):
        for j in range(Q):
            @pl.when(me < stages - 1)
            def _():
                f_copy(m, j).wait_send()

            @pl.when(me > 0)
            def _():
                b_copy(m, j).wait_send()

    for store in stores:
        store.wait()


def solution(mesh):
    stages = mesh.shape["pp"]

    def step(x, dy, w_gate, w_up, w_down):
        micro, tokens, d = x.shape
        ff = w_gate.shape[2]
        bf16, f32 = jnp.bfloat16, jnp.float32
        anywhere = pl.BlockSpec(memory_space=pl.ANY)
        dma = pltpu.SemaphoreType.DMA
        outs = pl.pallas_call(
            functools.partial(kernel, stages),
            out_shape=(
                jax.ShapeDtypeStruct(w_gate.shape, bf16),
                jax.ShapeDtypeStruct(w_up.shape, bf16),
                jax.ShapeDtypeStruct(w_down.shape, bf16),
                jax.ShapeDtypeStruct((micro, 2, tokens, ff), f32),
                jax.ShapeDtypeStruct((micro, tokens, ff), bf16),
            ),
            in_specs=[anywhere] * 5,
            out_specs=(anywhere,) * 5,
            scratch_shapes=[
                pltpu.VMEM((d, ff), bf16),
                pltpu.VMEM((d, ff), bf16),
                pltpu.VMEM((ff, d), bf16),
                pltpu.VMEM((ff, d), bf16),
                pltpu.VMEM((ff, d), bf16),
                pltpu.VMEM((d, ff), bf16),
                pltpu.VMEM((d, ff), f32),
                pltpu.VMEM((d, ff), f32),
                pltpu.VMEM((d, ff), f32),
                pltpu.VMEM((NH, tokens, d), bf16),
                pltpu.VMEM((NG, tokens, d), bf16),
                pltpu.VMEM((2, tokens, d), bf16),
                pltpu.VMEM((2, tokens, d), bf16),
                pltpu.VMEM((2, 2, tokens, ff), f32),
                pltpu.VMEM((tokens, d), bf16),
                pltpu.VMEM((tokens, ff), bf16),
                pltpu.VMEM((tokens // COARSE, d), bf16),
                pltpu.VMEM((tokens, ff), bf16),
                pltpu.VMEM((ND, tokens, ff), bf16),
                pltpu.VMEM((ND, tokens, ff), bf16),
                pltpu.VMEM((ND, d, tokens), bf16),
                pltpu.VMEM((ND, d, tokens), bf16),
                dma((3,)),
                dma,
                dma,
                dma((NH * Q,)),
                dma((2 * Q,)),
                dma((NG * Q,)),
                dma((2 * Q,)),
                dma((2 * Q,)),
                dma((Q + 1,)),
                pltpu.SemaphoreType.REGULAR,
                pltpu.SemaphoreType.REGULAR,
            ],
            compiler_params=pltpu.CompilerParams(collective_id=0, has_side_effects=True, vmem_limit_bytes=67043328),
        )(x, dy, w_gate, w_up, w_down)
        return outs[:3]

    return jax.shard_map(
        step,
        mesh=mesh,
        in_specs=(P("rep", None, None),) * 2 + (P("pp", None, None),) * 3,
        out_specs=(P(("rep", "pp"), None, None),) * 3,
        check_vma=False,
    )
```

```python
import functools

import jax
import jax.numpy as jnp
from jax import lax
from jax.experimental import pallas as pl
from jax.experimental.pallas import tpu as pltpu
from jax.sharding import PartitionSpec as P

Q = 4
COARSE, FINE = 2, 4
FINE_F, FINE_B = 5, 4
NH = 14
NG = 3
ND = 2
TF, TB, TD, TW, TR = 256, 512, 256, 512, 64
EPS = 1e-6


def dot(a, b):
    return jnp.dot(a, b, preferred_element_type=jnp.float32)


def dot_t(a, b):
    return lax.dot_general(a, b, (((1,), (1,)), ((), ())), preferred_element_type=jnp.float32)


def norm(h):
    wide = h.astype(jnp.float32)
    scale = lax.rsqrt(jnp.mean(wide * wide, -1, keepdims=True) + EPS)
    return wide, scale


def kernel(stages, x_hbm, dy_hbm, wg_hbm, wu_hbm, wd_hbm, og_hbm, ou_hbm, od_hbm, spill, acts, wg, wu, wd, wgt, wut, wdt, tg, tu, td, hbuf, gbuf, fsend,
           bsend, pool, a_v, act_v, by_a_v, sa, sg, su, at, dt, wsem, xsem, ysem, frecv, fsent, brecv, bsent, keepsem, backsem, fcred, bcred):
    micro, tokens, d = x_hbm.shape
    ff = wg.shape[1]
    part = tokens // Q
    me = lax.axis_index("pp")
    first, last = me == 0, me == stages - 1
    behind = stages - 1 - me
    warm = jnp.minimum(1 + lax.div(behind * 3, 2) + jnp.where(me < 2, 4, 0), NH - 1)
    late = jnp.where((me >= 2) & (me < stages - 1), ND - 1, 0)
    resident = warm <= 2

    loads = [pltpu.make_async_copy(src.at[0], dst, wsem.at[i]) for i, (src, dst) in enumerate(((wg_hbm, wg), (wu_hbm, wu), (wd_hbm, wd)))]
    for load in loads:
        load.start()

    def rows(j, count=1):
        return pl.ds(pl.multiple_of(j * part, part), count * part)

    def x_copy(m):
        return pltpu.make_async_copy(x_hbm.at[m], hbuf.at[lax.rem(m, NH)], xsem)

    def dy_copy(m):
        return pltpu.make_async_copy(dy_hbm.at[m], gbuf.at[lax.rem(m, NG)], ysem)

    @pl.when(first)
    def _():
        x_copy(0).start()

    @pl.when(last)
    def _():
        dy_copy(0).start()

    barrier = pltpu.get_barrier_semaphore()

    @pl.when(me > 0)
    def _():
        pl.semaphore_signal(barrier, inc=1, device_id={"pp": me - 1})

    @pl.when(me < stages - 1)
    def _():
        pl.semaphore_signal(barrier, inc=1, device_id={"pp": me + 1})

    pl.semaphore_wait(barrier, jnp.where(first | last, 1, 2))

    def f_copy(m, j):
        out, slot = lax.rem(m, 2), lax.rem(m, NH)
        return pltpu.make_async_remote_copy(
            src_ref=fsend.at[out, rows(j)], dst_ref=hbuf.at[slot, rows(j)], send_sem=fsent.at[out * Q + j], recv_sem=frecv.at[slot * Q + j],
            device_id={"pp": me + 1},
        )

    def b_copy(m, j):
        out, slot = lax.rem(m, 2), lax.rem(m, NG)
        return pltpu.make_async_remote_copy(
            src_ref=bsend.at[out, rows(j)], dst_ref=gbuf.at[slot, rows(j)], send_sem=bsent.at[out * Q + j], recv_sem=brecv.at[slot * Q + j],
            device_id={"pp": me - 1},
        )

    def keep_copy(m, j):
        return pltpu.make_async_copy(pool.at[0, :, rows(j)], spill.at[m, :, rows(j)], keepsem.at[j])

    def act_copy(m, j):
        return pltpu.make_async_copy(act_v.at[rows(j)], acts.at[m, rows(j)], keepsem.at[Q + j])

    def back_copy(m, j):
        return pltpu.make_async_copy(spill.at[m, :, rows(j)], pool.at[1, :, rows(j)], backsem.at[j])

    def sa_copy(m):
        return pltpu.make_async_copy(acts.at[m], sa, backsem.at[Q])

    for load in loads:
        load.wait()

    def forward(m, blocks):
        slot, out, each = lax.rem(m, NH), lax.rem(m, 2), Q // blocks
        place = jnp.where(resident, lax.rem(m, 2), 0)

        def hidden(r):
            wide, scale = norm(hbuf[slot, r])
            a = (wide * scale).astype(jnp.bfloat16)
            a_v[r, :] = a
            for n in range(0, ff, TF):
                n = slice(n, n + TF)
                gate, up = dot(a_v[r, :], wg[:, n]), dot(a_v[r, :], wu[:, n])
                s = jax.nn.sigmoid(gate)
                silu = gate * s
                pool[place, 0, r, n] = silu
                pool[place, 1, r, n] = up * (s + silu * (1.0 - s))
                act_v[r, n] = (silu * up).astype(jnp.bfloat16)

        def block(i, _):
            r = rows(i * each, each)

            @pl.when(me > 0)
            def _():
                for j in range(each):
                    f_copy(m, i * each + j).wait_recv()

            @pl.when((me < stages - 1) & (m >= 2))
            def _():
                for j in range(each):
                    f_copy(m - 2, i * each + j).wait_send()

            @pl.when(last)
            def _():
                hidden(r)

            @pl.when(me < stages - 1)
            def _():
                hidden(r)
                if blocks == COARSE:
                    fsend[out, r] = hbuf[slot, r] + dot_t(wdt[...], act_v[r, :]).astype(jnp.bfloat16).T
                else:
                    for n in range(0, d, TD):
                        n = slice(n, min(n + TD, d))
                        fsend[out, r, n] = hbuf[slot, r, n] + dot(act_v[r, :], wd[:, n]).astype(jnp.bfloat16)
                for j in range(each):
                    f_copy(m, i * each + j).start()

            for j in range(each):
                act_copy(m, i * each + j).start()

            @pl.when(jnp.logical_not(resident))
            def _():
                for j in range(each):
                    keep_copy(m, i * each + j).start()

            return 0

        lax.fori_loop(0, blocks, block, 0)

    def forwards(m):
        @pl.when(first)
        def _():
            x_copy(m).wait()

            @pl.when(m + 1 < micro)
            def _():
                x_copy(m + 1).start()

        @pl.when((me < stages - 1) & (m >= NH))
        def _():
            pl.semaphore_wait(fcred, 1)

        @pl.when(m < FINE_F)
        def _():
            forward(m, FINE)

        @pl.when(m >= FINE_F)
        def _():
            forward(m, COARSE)

    def backward(m, blocks):
        slot, hslot, q, out, each = lax.rem(m, NG), lax.rem(m, NH), lax.rem(m, ND), lax.rem(m, 2), Q // blocks
        place = jnp.where(resident, lax.rem(m, 2), 1)

        def hidden(r):
            for n in range(0, ff, TB):
                n = slice(n, n + TB)
                by_act = dot(gbuf[slot, r], wdt[:, n]).astype(jnp.bfloat16).astype(jnp.float32)
                su[q, r, n] = (by_act * pool[place, 0, r, n]).astype(jnp.bfloat16)
                sg[q, r, n] = (by_act * pool[place, 1, r, n]).astype(jnp.bfloat16)
            wide, scale = norm(hbuf[hslot, r])
            at[q, :, r] = (wide * scale).astype(jnp.bfloat16).T
            dt[q, :, r] = gbuf[slot, r].T

        def block(i, _):
            r = rows(i * each, each)

            @pl.when(me < stages - 1)
            def _():
                for j in range(each):
                    b_copy(m, i * each + j).wait_recv()

            @pl.when((me > 0) & (m >= 2))
            def _():
                for j in range(each):
                    b_copy(m - 2, i * each + j).wait_send()

            @pl.when(jnp.logical_not(resident))
            def _():
                for j in range(each):
                    back_copy(m, i * each + j).wait()

            @pl.when(first)
            def _():
                hidden(r)

            @pl.when(me > 0)
            def _():
                hidden(r)
                if blocks == COARSE:
                    by_at = dot_t(wg[...], sg[q, r, :]).astype(jnp.bfloat16) + dot_t(wu[...], su[q, r, :]).astype(jnp.bfloat16)
                    by_a_v[...] = by_at.T
                else:
                    for n in range(0, d, TD):
                        n = slice(n, min(n + TD, d))
                        by_a = dot(sg[q, r, :], wgt[:, n]).astype(jnp.bfloat16) + dot(su[q, r, :], wut[:, n]).astype(jnp.bfloat16)
                        by_a_v[0 : each * part, n] = by_a
                for p in range(0, each * part, TR):
                    o = pl.ds(pl.multiple_of(i * each * part + p, TR), TR)
                    by_a = by_a_v[p : p + TR, :].astype(jnp.float32)
                    wide, scale = norm(hbuf[hslot, o])
                    by_scale = jnp.sum(by_a * wide, -1, keepdims=True)
                    by_wide = by_a * scale - wide * (by_scale * (scale * scale * scale) * (1.0 / d))
                    bsend[out, o] = by_wide.astype(jnp.bfloat16) + gbuf[slot, o]
                for j in range(each):
                    b_copy(m, i * each + j).start()

            return 0

        lax.fori_loop(0, blocks, block, 0)

    def backwards(m):
        @pl.when(last)
        def _():
            dy_copy(m).wait()

            @pl.when(m + 1 < micro)
            def _():
                dy_copy(m + 1).start()

        @pl.when((me > 0) & (m >= NG))
        def _():
            pl.semaphore_wait(bcred, 1)

        @pl.when(m < micro - FINE_B)
        def _():
            backward(m, COARSE)

        @pl.when(m >= micro - FINE_B)
        def _():
            backward(m, FINE)

        @pl.when((me > 0) & (m + NH < micro))
        def _():
            pl.semaphore_signal(fcred, inc=1, device_id={"pp": me - 1})

        @pl.when((me < stages - 1) & (m + NG < micro))
        def _():
            pl.semaphore_signal(bcred, inc=1, device_id={"pp": me + 1})

    def term(total, left, right):
        for n in range(0, ff, TW):
            n = slice(n, n + TW)
            total[:, n] += dot(left[...], right[:, n]).astype(jnp.bfloat16).astype(jnp.float32)

    stores = [pltpu.make_async_copy(src, dst.at[0], wsem.at[i]) for i, (src, dst) in enumerate(((wg, og_hbm), (wu, ou_hbm), (wd, od_hbm)))]

    def step(t, _):
        f, b = t, t - warm
        w = b - late
        q = lax.rem(w + ND * micro, ND)
        f_on, w_on, more = f < micro, (w >= 0) & (w < micro), (b + 1 >= 0) & (b + 1 < micro)

        @pl.when((b >= 0) & (b < micro))
        def _():
            backwards(b)

        @pl.when(more & jnp.logical_not(resident))
        def _():
            for j in range(Q):
                back_copy(b + 1, j).start()

        @pl.when(f_on)
        def _():
            forwards(f)

        @pl.when(t == 0)
        def _():
            for total in (tg, tu, td):
                total[...] = jnp.zeros_like(total)
            wgt[...] = wg[...].T
            wut[...] = wu[...].T
            wdt[...] = wd[...].T

        @pl.when(w_on & (w < micro - 1))
        def _():
            sa_copy(w).wait()
            term(tg, at.at[q], sg.at[q])
            term(tu, at.at[q], su.at[q])
            term(td, dt.at[q], sa)

        @pl.when(w == micro - 1)
        def _():
            sa_copy(w).wait()
            term(tg, at.at[q], sg.at[q])
            wg[...] = tg[...].astype(jnp.bfloat16)
            stores[0].start()
            term(tu, at.at[q], su.at[q])
            wu[...] = tu[...].astype(jnp.bfloat16)
            stores[1].start()
            term(td, dt.at[q], sa)
            wd[...] = td[...].astype(jnp.bfloat16).T
            stores[2].start()

        @pl.when(f_on)
        def _():
            for j in range(Q):
                act_copy(f, j).wait()

            @pl.when(jnp.logical_not(resident))
            def _():
                for j in range(Q):
                    keep_copy(f, j).wait()

        @pl.when((w + 1 >= 0) & (w + 1 < micro))
        def _():
            sa_copy(w + 1).start()

        return 0

    lax.fori_loop(0, micro + warm + late, step, 0)

    for m in (micro - 2, micro - 1):
        for j in range(Q):
            @pl.when(me < stages - 1)
            def _():
                f_copy(m, j).wait_send()

            @pl.when(me > 0)
            def _():
                b_copy(m, j).wait_send()

    for store in stores:
        store.wait()


def solution(mesh):
    stages = mesh.shape["pp"]

    def step(x, dy, w_gate, w_up, w_down):
        micro, tokens, d = x.shape
        ff = w_gate.shape[2]
        bf16, f32 = jnp.bfloat16, jnp.float32
        anywhere = pl.BlockSpec(memory_space=pl.ANY)
        dma = pltpu.SemaphoreType.DMA
        outs = pl.pallas_call(
            functools.partial(kernel, stages),
            out_shape=(
                jax.ShapeDtypeStruct(w_gate.shape, bf16),
                jax.ShapeDtypeStruct(w_up.shape, bf16),
                jax.ShapeDtypeStruct(w_down.shape, bf16),
                jax.ShapeDtypeStruct((micro, 2, tokens, ff), f32),
                jax.ShapeDtypeStruct((micro, tokens, ff), bf16),
            ),
            in_specs=[anywhere] * 5,
            out_specs=(anywhere,) * 5,
            scratch_shapes=[
                pltpu.VMEM((d, ff), bf16),
                pltpu.VMEM((d, ff), bf16),
                pltpu.VMEM((ff, d), bf16),
                pltpu.VMEM((ff, d), bf16),
                pltpu.VMEM((ff, d), bf16),
                pltpu.VMEM((d, ff), bf16),
                pltpu.VMEM((d, ff), f32),
                pltpu.VMEM((d, ff), f32),
                pltpu.VMEM((d, ff), f32),
                pltpu.VMEM((NH, tokens, d), bf16),
                pltpu.VMEM((NG, tokens, d), bf16),
                pltpu.VMEM((2, tokens, d), bf16),
                pltpu.VMEM((2, tokens, d), bf16),
                pltpu.VMEM((2, 2, tokens, ff), f32),
                pltpu.VMEM((tokens, d), bf16),
                pltpu.VMEM((tokens, ff), bf16),
                pltpu.VMEM((tokens // COARSE, d), bf16),
                pltpu.VMEM((tokens, ff), bf16),
                pltpu.VMEM((ND, tokens, ff), bf16),
                pltpu.VMEM((ND, tokens, ff), bf16),
                pltpu.VMEM((ND, d, tokens), bf16),
                pltpu.VMEM((ND, d, tokens), bf16),
                dma((3,)),
                dma,
                dma,
                dma((NH * Q,)),
                dma((2 * Q,)),
                dma((NG * Q,)),
                dma((2 * Q,)),
                dma((2 * Q,)),
                dma((Q + 1,)),
                pltpu.SemaphoreType.REGULAR,
                pltpu.SemaphoreType.REGULAR,
            ],
            compiler_params=pltpu.CompilerParams(collective_id=0, has_side_effects=True, vmem_limit_bytes=67043328),
        )(x, dy, w_gate, w_up, w_down)
        return outs[:3]

    return jax.shard_map(
        step,
        mesh=mesh,
        in_specs=(P("rep", None, None),) * 2 + (P("pp", None, None),) * 3,
        out_specs=(P(("rep", "pp"), None, None),) * 3,
        check_vma=False,
    )
```
